128 devices in a mesh: rep: 1, data: 16 (over z, y), expert: 8 (over x, core).
Axes of the slice: x: 4, y: 4, z: 4, core: 2. Of those that a mesh axis runs over, the one named last changes fastest.
Arguments:
- x_in: bfloat16 [2, 131072, 768], P(None, ('rep', 'expert', 'data'))
- expert_idx: int32 [2, 131072, 1], P(None, ('rep', 'expert', 'data'))
- gate_wt: float32 [2, 131072, 1], P(None, ('rep', 'expert', 'data'))
- w_gate: bfloat16 [32, 768, 3072], P('expert', 'data')
- w_up: bfloat16 [32, 768, 3072], P('expert', 'data')
- w_down: bfloat16 [32, 3072, 768], P('expert', None, 'data')
Outputs:
- output: bfloat16 [2, 131072, 768], P(None, ('rep', 'expert', 'data'))
All inputs are finite; a program needn't handle non-finite values.
Results may differ from the reference program's by a relative error of at most 0.001.
Values are sent between devices in bfloat16 or wider.
A program may use at most 1 GiB of HBM per device.

```python
import jax
import jax.numpy as jnp
from jax import lax

D_MODEL = 768
FF = 3072
N_EXP = 32
TOP = 1
TOK_LOC = 1024
EXPERT_DEVS = 8
DATA_DEVS = 16
CAP = 40


def draw_routing(route_key):
    dev_count = EXPERT_DEVS * DATA_DEVS
    key_noise, key_bias, key_hot, key_perm = jax.random.split(route_key, 4)
    draw_noise = jax.random.randint(key_noise, (2, dev_count, TOK_LOC, N_EXP), 0, 4096)
    exp_bias = jax.random.randint(key_bias, (2, 1, 1, N_EXP), 0, 1024)
    hot_id = jax.random.randint(key_hot, (2, dev_count, 1, 1), 0, N_EXP)
    perm_keys = jax.random.split(key_perm, 2 * dev_count)
    tok_rank = jax.vmap(lambda sub_key: jax.random.permutation(sub_key, TOK_LOC))(perm_keys)
    tok_rank = tok_rank.reshape(2, dev_count, TOK_LOC, 1)
    hot_count = min(TOK_LOC, CAP + CAP // 4)
    expert_ids = jnp.arange(N_EXP, dtype=jnp.int32)
    forced = jnp.logical_and(tok_rank < hot_count, expert_ids == hot_id).astype(jnp.int32)
    int_score = (draw_noise + exp_bias + forced * 8192) * N_EXP + expert_ids
    chosen = lax.top_k(int_score, TOP)[1].astype(jnp.int32)
    return chosen.reshape(2, dev_count * TOK_LOC, TOP)


def setup_inputs(seed: int = 0, part: int = 0) -> dict:
    base_key = jax.random.key(seed)
    shared_key, token_key = jax.random.split(base_key)
    part_key = jax.random.fold_in(token_key, part)
    key_x, key_route, key_gate = jax.random.split(part_key, 3)
    key_wg, key_wu, key_wd = jax.random.split(shared_key, 3)
    tok_all = EXPERT_DEVS * DATA_DEVS * TOK_LOC
    x_in = jax.random.normal(key_x, (2, tok_all, D_MODEL), jnp.float32).astype(jnp.bfloat16)
    expert_idx = draw_routing(key_route)
    gate_wt = jax.random.uniform(key_gate, (2, tok_all, TOP), jnp.float32, 0.2, 0.8)
    w_gate = (jax.random.normal(key_wg, (N_EXP, D_MODEL, FF), jnp.float32) * D_MODEL ** -0.5).astype(jnp.bfloat16)
    w_up = (jax.random.normal(key_wu, (N_EXP, D_MODEL, FF), jnp.float32) * D_MODEL ** -0.5).astype(jnp.bfloat16)
    w_down = (jax.random.normal(key_wd, (N_EXP, FF, D_MODEL), jnp.float32) * (1.5 * FF ** -0.5)).astype(jnp.bfloat16)
    return {'x_in': x_in, 'expert_idx': expert_idx, 'gate_wt': gate_wt, 'w_gate': w_gate, 'w_up': w_up, 'w_down': w_down}


def slot_table(ids_block):
    flat_ids = ids_block.reshape(-1)
    one_hot = (flat_ids[:, None] == jnp.arange(N_EXP, dtype=jnp.int32)[None, :]).astype(jnp.int32)
    slot_of = jnp.sum((jnp.cumsum(one_hot, axis=0) - one_hot) * one_hot, axis=1)
    return flat_ids, slot_of


def expert_ffn(rows_in, wg_one, wu_one, wd_one):
    gate_pre = jnp.dot(rows_in, wg_one, preferred_element_type=jnp.float32)
    up_pre = jnp.dot(rows_in, wu_one, preferred_element_type=jnp.float32)
    hidden = (jax.nn.silu(gate_pre) * up_pre).astype(jnp.bfloat16)
    return jnp.dot(hidden, wd_one, preferred_element_type=jnp.float32).astype(jnp.bfloat16)


def moe_micro(x_mb, idx_mb, gate_mb, w_gate, w_up, w_down):
    dev_count = EXPERT_DEVS * DATA_DEVS
    pair_count = TOK_LOC * TOP
    slot_total = N_EXP * CAP
    x_blocks = x_mb.reshape(dev_count, TOK_LOC, D_MODEL)
    flat_ids, slot_of = jax.vmap(slot_table)(idx_mb.reshape(dev_count, TOK_LOC, TOP))
    is_kept = slot_of < CAP
    dest_pos = jnp.where(is_kept, flat_ids * CAP + slot_of, slot_total)
    pair_ids = jnp.arange(pair_count, dtype=jnp.int32)
    source_of = jax.vmap(lambda dest_row: jnp.full((slot_total,), pair_count, jnp.int32).at[dest_row].set(pair_ids, mode='drop'))(dest_pos)
    tok_of = jnp.minimum(source_of // TOP, TOK_LOC - 1)
    buffers = jax.vmap(lambda x_blk, tok_row: x_blk[tok_row])(x_blocks, tok_of)
    buffers = jnp.where((source_of < pair_count)[:, :, None], buffers, jnp.zeros((), jnp.bfloat16))
    per_expert = buffers.reshape(dev_count, N_EXP, CAP, D_MODEL).transpose(1, 0, 2, 3).reshape(N_EXP, dev_count * CAP, D_MODEL)
    expert_out = lax.map(lambda expert_args: expert_ffn(expert_args[0], expert_args[1], expert_args[2], expert_args[3]), (per_expert, w_gate, w_up, w_down))
    back_rows = expert_out.reshape(N_EXP, dev_count, CAP, D_MODEL).transpose(1, 0, 2, 3).reshape(dev_count, slot_total, D_MODEL)
    pair_out = jax.vmap(lambda back_blk, pos_row: back_blk[pos_row])(back_rows, jnp.minimum(dest_pos, slot_total - 1))
    pair_out = pair_out.reshape(dev_count, TOK_LOC, TOP, D_MODEL).astype(jnp.float32)
    weight = jnp.where(is_kept.reshape(dev_count, TOK_LOC, TOP), gate_mb.reshape(dev_count, TOK_LOC, TOP), 0.0)
    mix_sum = jnp.sum(pair_out * weight[:, :, :, None], axis=2)
    y_blocks = (x_blocks.astype(jnp.float32) + mix_sum).astype(jnp.bfloat16)
    return y_blocks.reshape(dev_count * TOK_LOC, D_MODEL)


def reference(x_in, expert_idx, gate_wt, w_gate, w_up, w_down):
    return lax.map(lambda mb_args: moe_micro(mb_args[0], mb_args[1], mb_args[2], w_gate, w_up, w_down), (x_in, expert_idx, gate_wt))
```

```python
import functools

import jax
import jax.numpy as jnp
from jax import lax
from jax.experimental import pallas as pl
from jax.experimental.pallas import tpu as pltpu
from jax.sharding import PartitionSpec as P

MESH = pl.DeviceIdType.MESH
N_CHUNK = 3
N_EXP = 32
CAP = 40
ROWS = 2 * CAP
D = 768
FF = 3072
HALF = FF // 2
TOK = 1024
SL = 48


def moe_kernel(x_ref, idx_ref, gate_ref, wg, wu, wd, y_ref,
               W, ST, S, Xr, acc, O, B, dT, gT,
               s1, s2, s3, xs, rs, ss1, ss2, ssx):
    fc = HALF // N_CHUNK
    d = lax.axis_index('data')
    g = lax.axis_index('expert')
    z, y = lax.div(d, 4), lax.rem(d, 4)
    xx, c = lax.div(g, 2), lax.rem(g, 2)
    own_p = lax.div(y, 2)
    yo = 3 - y
    yi = y + 1 - 2 * lax.rem(y, 2)
    sib = 1 - c

    def dev(zv, yv, xv, cv):
        return {'data': zv * 4 + yv, 'expert': xv * 2 + cv}

    def remote(src, dst, send, recv, to):
        return pltpu.make_async_remote_copy(src_ref=src, dst_ref=dst, send_sem=send, recv_sem=recv, device_id=to, device_id_type=MESH)

    def wait_bytes(ref, sem):
        pltpu.make_async_copy(ref, ref, sem).wait()

    bsem = pltpu.get_barrier_semaphore()
    n_peer = 0
    for dx in range(4):
        for dz in range(4):
            for b in range(2):
                if dx or dz or b:
                    pl.semaphore_signal(bsem, inc=1, device_id=dev(lax.rem(z + dz, 4), yo if b else y, lax.rem(xx + dx, 4), c), device_id_type=MESH)
                    n_peer += 1
    for dz in range(4):
        pl.semaphore_signal(bsem, inc=1, device_id=dev(lax.rem(z + dz, 4), y, xx, sib), device_id_type=MESH)
        n_peer += 1
    pl.semaphore_signal(bsem, inc=1, device_id=dev(z, yi, xx, c), device_id_type=MESH)
    n_peer += 1
    pl.semaphore_wait(bsem, n_peer)

    def send_w(j):
        for a in range(2):
            zt = 2 * c + a
            for o in range(2):
                l = 2 * a + (1 - own_p if o else own_p)
                for k in range(2):
                    local = jnp.logical_and(zt == z, c == k)
                    for t, w in enumerate((wg, wu, wd)):
                        src = w.at[l, :, pl.ds(k * HALF + j * fc, fc)]
                        dst = ST.at[j, t, z] if o else W.at[k, j, t, z, y]

                        @pl.when(local)
                        def _():
                            pltpu.make_async_copy(src, dst, s1.at[o, j]).start()

                        @pl.when(jnp.logical_not(local))
                        def _():
                            remote(src, dst, ss1.at[t], s1.at[o, j], dev(zt, y, xx, k)).start()

    def col(j, yv):
        return W.at[c, j, :, :, yv]

    def to_sib(j, yv):
        remote(col(j, yv), col(j, yv), ss2.at[2], s3.at[j], dev(z, y, xx, sib)).start()

    def step_a(j):
        wait_bytes(ST.at[j], s1.at[1, j])
        remote(ST.at[j], col(j, y), ss2.at[0], s2.at[0, j], dev(z, yo, xx, c)).start()
        wait_bytes(col(j, y), s1.at[0, j])
        remote(col(j, y), col(j, y), ss2.at[1], s2.at[1, j], dev(z, yi, xx, c)).start()
        to_sib(j, y)

    def step_b(j):
        wait_bytes(col(j, yo), s2.at[0, j])
        remote(col(j, yo), col(j, yo), ss2.at[1], s2.at[2, j], dev(z, yi, xx, c)).start()
        to_sib(j, yo)

    def step_c(j):
        wait_bytes(col(j, yi), s2.at[1, j])
        to_sib(j, yi)

    def step_d(j):
        wait_bytes(col(j, 3 - yi), s2.at[2, j])
        to_sib(j, 3 - yi)

    def step_e(j):
        wait_bytes(W.at[sib, j], s3.at[j])

    send_w(0)

    earlier = (lax.broadcasted_iota(jnp.int32, (TOK, TOK), 0) < lax.broadcasted_iota(jnp.int32, (TOK, TOK), 1)).astype(jnp.bfloat16)
    dest = []
    for m in range(2):
        ids = idx_ref[m]
        hot = (lax.broadcasted_iota(jnp.int32, (N_EXP, TOK), 0) == ids).astype(jnp.float32)
        before = jnp.dot(hot.astype(jnp.bfloat16), earlier, preferred_element_type=jnp.float32)
        slot = jnp.sum(hot * before, axis=0, keepdims=True)
        kept = slot < CAP
        dest.append(jnp.where(kept, ids.astype(jnp.float32) * CAP + slot, -1.0))
    e_me = 8 * xx + 2 * z + own_p
    for dx in range(4):
        xt = lax.rem(xx + dx, 4)
        parts = []
        for m in range(2):
            pos = (lax.broadcasted_iota(jnp.int32, (8 * CAP, TOK), 0) + xt * (8 * CAP)).astype(jnp.float32)
            pick = (pos == dest[m]).astype(jnp.bfloat16)
            parts.append(jnp.dot(pick, x_ref[m], preferred_element_type=jnp.float32).reshape(8, CAP, D))
        S[pl.ds(xt * 8, 8)] = jnp.concatenate(parts, axis=1).astype(jnp.bfloat16)
        for dz in range(4):
            zt = lax.rem(z + dz, 4)
            for b in range(2):
                yt = yo if b else y
                e = 8 * xt + 2 * zt + lax.div(yt, 2)
                s = (dx * 4 + dz) * 2 + b
                if s == 0:
                    Xr[0] = S[e]
                else:
                    remote(S.at[e], Xr.at[s], ssx.at[0], xs.at[dx], dev(zt, yt, xt, c)).start()
        if dx + 1 < N_CHUNK:
            send_w(dx + 1)
    for j in range(5, N_CHUNK):
        send_w(j)
    for m in range(2):
        dT[m] = jnp.broadcast_to(dest[m], (128, TOK)).T
        gT[m] = jnp.broadcast_to(gate_ref[m], (128, TOK)).T

    def mlp(k, j, r):
        rows = Xr[pl.ds(r * 8, 8)].reshape(8 * ROWS, D)
        gate_pre = jnp.dot(rows, W[k, j, 0].reshape(D, fc), preferred_element_type=jnp.float32)
        up_pre = jnp.dot(rows, W[k, j, 1].reshape(D, fc), preferred_element_type=jnp.float32)
        hidden = (jax.nn.silu(gate_pre) * up_pre).astype(jnp.bfloat16)
        return lax.dot_general(hidden, W[k, j, 2].reshape(D, fc), (((1,), (1,)), ((), ())), preferred_element_type=jnp.float32)

    def wait_rows(r):
        if r == 0:
            wait_bytes(Xr.at[pl.ds(1, 7)], xs.at[0])
        else:
            wait_bytes(Xr.at[pl.ds(r * 8, 8)], xs.at[r])

    step_a(0)
    step_b(0)
    step_c(0)
    for j in range(N_CHUNK):
        if j + 1 < N_CHUNK:
            step_a(j + 1)
        step_d(j)
        if j == 0:
            for r in range(4):
                wait_rows(r)
                acc[r] = mlp(c, 0, r)
        else:
            @pl.loop(0, 4)
            def _(r):
                acc[r] += mlp(c, j, r)
        if j + 1 < N_CHUNK:
            step_b(j + 1)
            step_c(j + 1)
        step_e(j)
        if j + 1 < N_CHUNK:
            @pl.loop(0, 4)
            def _(r):
                acc[r] += mlp(sib, j, r)
    for r in range(4):
        O[pl.ds(r * 8, 8)] = (acc[r] + mlp(sib, N_CHUNK - 1, r)).astype(jnp.bfloat16).reshape(8, ROWS, D)
        for dz in range(4):
            for b in range(2):
                s = (r * 4 + dz) * 2 + b
                if s == 0:
                    B[e_me] = O[0]
                else:
                    remote(O.at[s], B.at[e_me], ssx.at[1], rs.at[r],
                           dev(lax.rem(z + 4 - dz, 4), yo if b else y, lax.rem(xx + 4 - r, 4), c)).start()

    wait_bytes(B.at[pl.ds(0, 7)], rs.at[0])
    for r in range(1, 4):
        wait_bytes(B.at[pl.ds(r * 8, 8)], rs.at[r])
    for m in range(2):
        for q in range(4):
            back = B[pl.ds(q * 8, 8)].astype(jnp.float32)[:, m * CAP:(m + 1) * CAP].reshape(4, ROWS, D)
            Xr[pl.ds(m * 16 + q * 4, 4)] = back.astype(jnp.bfloat16)
    for m in range(2):
        @pl.loop(0, 4)
        def _(i):
            at = pl.ds(pl.multiple_of(i * 256, 256), 256)
            dest_col = dT[m, at]
            pick = jnp.concatenate(
                [(dest_col == (lax.broadcasted_iota(jnp.int32, (256, 128), 1) + 128 * v).astype(jnp.float32)).astype(jnp.bfloat16)
                 for v in range(10)], axis=1)
            back = Xr[pl.ds(m * 16, 16)].reshape(N_EXP * CAP, D)
            mixed = jnp.dot(pick, back, preferred_element_type=jnp.float32)
            weight = jnp.concatenate([gT[m, at]] * (D // 128), axis=1)
            y_ref[m, at] = (x_ref[m, at].astype(jnp.float32) + weight * mixed).astype(jnp.bfloat16)

    has_local = lax.div(z, 2) == c
    for t, w in enumerate((wg, wu, wd)):
        @pl.when(has_local)
        def _():
            wait_bytes(w.at[pl.ds(0, 3)], ss1.at[t])

        @pl.when(jnp.logical_not(has_local))
        def _():
            wait_bytes(w, ss1.at[t])
    wait_bytes(ST, ss2.at[0])
    wait_bytes(W.at[0, :, :, :, pl.ds(0, 2)], ss2.at[1])
    wait_bytes(W.at[0], ss2.at[2])
    wait_bytes(S.at[pl.ds(0, 31)], ssx.at[0])
    wait_bytes(O.at[pl.ds(0, 31)], ssx.at[1])


def solution(mesh):
    row_spec = P(None, ('rep', 'expert', 'data'), None)
    up_spec = P('expert', 'data', None)
    down_spec = P('expert', None, 'data')
    fc = HALF // N_CHUNK
    bf16 = jnp.bfloat16

    def per_device(x_loc, idx_loc, gate_loc, wg_loc, wu_loc, wd_loc):
        vmem = pl.BlockSpec(memory_space=pltpu.VMEM)
        hbm = pl.BlockSpec(memory_space=pl.ANY)
        dma = pltpu.SemaphoreType.DMA
        return pl.pallas_call(
            moe_kernel,
            out_shape=jax.ShapeDtypeStruct((2, TOK, D), bf16),
            in_specs=[vmem, vmem, vmem, hbm, hbm, hbm],
            out_specs=vmem,
            scratch_shapes=[
                pltpu.VMEM((2, N_CHUNK, 3, 4, 4, SL, fc), bf16),
                pltpu.VMEM((N_CHUNK, 3, 4, SL, fc), bf16),
                pltpu.VMEM((N_EXP, ROWS, D), bf16),
                pltpu.VMEM((N_EXP, ROWS, D), bf16),
                pltpu.VMEM((4, 8 * ROWS, D), jnp.float32),
                pltpu.VMEM((N_EXP, ROWS, D), bf16),
                pltpu.VMEM((N_EXP, ROWS, D), bf16),
                pltpu.VMEM((2, TOK, 128), jnp.float32),
                pltpu.VMEM((2, TOK, 128), jnp.float32),
                dma((2, N_CHUNK)), dma((3, N_CHUNK)), dma((N_CHUNK,)), dma((4,)), dma((4,)),
                dma((3,)), dma((3,)), dma((2,)),
            ],
            compiler_params=pltpu.CompilerParams(collective_id=0, has_side_effects=True, vmem_limit_bytes=67043328),
            name='moe',
        )(x_loc, idx_loc.reshape(2, 1, TOK), gate_loc.reshape(2, 1, TOK), wg_loc, wu_loc, wd_loc.transpose(0, 2, 1))

    return jax.shard_map(per_device, mesh=mesh, in_specs=(row_spec, row_spec, row_spec, up_spec, up_spec, down_spec), out_specs=row_spec, check_vma=False)
```

```python
import functools

import jax
import jax.numpy as jnp
from jax import lax
from jax.experimental import pallas as pl
from jax.experimental.pallas import tpu as pltpu
from jax.sharding import PartitionSpec as P

MESH = pl.DeviceIdType.MESH
N_CHUNK = 6
N_EXP = 32
CAP = 40
ROWS = 2 * CAP
D = 768
ZY = ((0, 0), (2, 1), (1, 0), (3, 1), (3, 0), (1, 1), (0, 1), (2, 0))
HEAD = ('W0', 'W1', 'W2', 'W3', 'W4', 'W5')
SCHED = (
    'P0', 'X0', 'P1', 'X1', 'A0', 'P2', 'X2', 'A1', 'P3', 'X3', 'Z', 'C0', 'B0', 'A2', 'C1', 'B1', 'A3', 'U0', 'D0',
    'B2', 'A4', 'U1', 'C2', 'B3', 'A5', 'U2', 'E0', 'D1', 'B4', 'U3', 'C3', 'B5', 'R0', 'K0101', 'E1', 'K1201', 'D2',
    'C4', 'E2', 'K2301', 'D3', 'C5', 'E3', 'K3401', 'D4', 'E4', 'K4501', 'R1', 'K0212', 'D5', 'R2', 'R3', 'E5',
)
DONE = (5, 2, 0, 0)
FF = 3072
HALF = FF // 2
TOK = 1024
SL = 48


def moe_kernel(x_ref, idx_ref, gate_ref, wg, wu, wd, y_ref,
               W, ST, S, T1, R1, Xr, acc, B, dT, gT,
               s1, s2, s3, xs1, xs2, rs1, rs2, ss1, ss2, ssx):
    fc = HALF // N_CHUNK
    d = lax.axis_index('data')
    g = lax.axis_index('expert')
    z, y = lax.div(d, 4), lax.rem(d, 4)
    xx, c = lax.div(g, 2), lax.rem(g, 2)
    own_p = lax.div(y, 2)
    yo = 3 - y
    yi = y + 1 - 2 * lax.rem(y, 2)
    sib = 1 - c

    def dev(zv, yv, xv, cv):
        return {'data': zv * 4 + yv, 'expert': xv * 2 + cv}

    def remote(src, dst, send, recv, to):
        return pltpu.make_async_remote_copy(src_ref=src, dst_ref=dst, send_sem=send, recv_sem=recv, device_id=to, device_id_type=MESH)

    def wait_bytes(ref, sem):
        pltpu.make_async_copy(ref, ref, sem).wait()

    bsem = pltpu.get_barrier_semaphore()
    n_peer = 10
    for dx in range(1, 4):
        pl.semaphore_signal(bsem, inc=1, device_id=dev(z, y, lax.rem(xx + dx, 4), c), device_id_type=MESH)
    for dz, b in ZY[1:]:
        pl.semaphore_signal(bsem, inc=1, device_id=dev(lax.rem(z + dz, 4), yo if b else y, xx, c), device_id_type=MESH)
    for dz in range(4):
        pl.semaphore_signal(bsem, inc=1, device_id=dev(lax.rem(z + dz, 4), y, xx, sib), device_id_type=MESH)
        n_peer += 1
    pl.semaphore_signal(bsem, inc=1, device_id=dev(z, yi, xx, c), device_id_type=MESH)
    n_peer += 1
    pl.semaphore_wait(bsem, n_peer)

    def send_w(j):
        for a in range(2):
            zt = 2 * c + a
            for o in range(2):
                l = 2 * a + (1 - own_p if o else own_p)
                for k in range(2):
                    local = jnp.logical_and(zt == z, c == k)
                    for t, w in enumerate((wg, wu, wd)):
                        src = w.at[l, :, pl.ds(k * HALF + j * fc, fc)]
                        dst = ST.at[j, t, z] if o else W.at[k, j, t, z, y]

                        @pl.when(local)
                        def _():
                            pltpu.make_async_copy(src, dst, s1.at[o, j]).start()

                        @pl.when(jnp.logical_not(local))
                        def _():
                            remote(src, dst, ss1.at[t], s1.at[o, j], dev(zt, y, xx, k)).start()

    def col(j, yv):
        return W.at[c, j, :, :, yv]

    def to_sib(j, yv):
        remote(col(j, yv), col(j, yv), ss2.at[2], s3.at[j], dev(z, y, xx, sib)).start()

    def step_a(j):
        wait_bytes(ST.at[j], s1.at[1, j])
        remote(ST.at[j], col(j, y), ss2.at[0], s2.at[0, j], dev(z, yo, xx, c)).start()
        wait_bytes(col(j, y), s1.at[0, j])
        remote(col(j, y), col(j, y), ss2.at[1], s2.at[1, j], dev(z, yi, xx, c)).start()
        to_sib(j, y)

    def step_b(j):
        wait_bytes(col(j, yo), s2.at[0, j])
        remote(col(j, yo), col(j, yo), ss2.at[1], s2.at[2, j], dev(z, yi, xx, c)).start()
        to_sib(j, yo)

    def step_c(j):
        wait_bytes(col(j, yi), s2.at[1, j])
        to_sib(j, yi)

    def step_d(j):
        wait_bytes(col(j, 3 - yi), s2.at[2, j])
        to_sib(j, 3 - yi)

    def step_e(j):
        wait_bytes(W.at[sib, j], s3.at[j])

    ops = dict(W=send_w, A=step_a, B=step_b, C=step_c, D=step_d, E=step_e)

    def run(plan):
        for word in plan:
            ops[word[0]](*[int(v) for v in word[1:]])

    run(HEAD)

    earlier = (lax.broadcasted_iota(jnp.int32, (TOK, TOK), 0) < lax.broadcasted_iota(jnp.int32, (TOK, TOK), 1)).astype(jnp.bfloat16)
    dest = []
    for m in range(2):
        e = idx_ref[m]
        step_x = lax.bitwise_and(lax.shift_right_logical(e, 3) - xx, 3)
        step_z = lax.bitwise_and(lax.shift_right_logical(e, 1) - z, 3)
        other = lax.bitwise_and(e + own_p, 1)
        ids = step_x
        for zb, (dz, b) in enumerate(ZY):
            ids = ids + jnp.where(step_z * 2 + other == dz * 2 + b, 4 * zb, 0)
        hot = (lax.broadcasted_iota(jnp.int32, (N_EXP, TOK), 0) == ids).astype(jnp.float32)
        before = jnp.dot(hot.astype(jnp.bfloat16), earlier, preferred_element_type=jnp.float32)
        slot = jnp.sum(hot * before, axis=0, keepdims=True)
        kept = slot < CAP
        dest.append(jnp.where(kept, ids.astype(jnp.float32) * CAP + slot, -1.0))
    def prep(i):
        parts = []
        for m in range(2):
            pos = (lax.broadcasted_iota(jnp.int32, (8 * CAP, TOK), 0) + i * (8 * CAP)).astype(jnp.float32)
            pick = (pos == dest[m]).astype(jnp.bfloat16)
            parts.append(jnp.dot(pick, x_ref[m], preferred_element_type=jnp.float32).reshape(8, CAP, D))
        rows = jnp.concatenate(parts, axis=1).astype(jnp.bfloat16).reshape(2, 4, ROWS, D)
        S[pl.ds(2 * i, 2)] = rows
        if i:
            T1[pl.ds(2 * i, 2), 0] = rows[:, 0]
        else:
            Xr[0, 0] = rows[0, 0]
            T1[1, 0] = rows[1, 0]

    def send_x(i):
        for zb in (2 * i, 2 * i + 1):
            for dx in (1, 3, 2):
                land = T1 if zb else Xr
                remote(S.at[zb, dx], land.at[zb, dx], ssx.at[0], xs1.at[i], dev(z, y, lax.rem(xx + dx, 4), c)).start()

    def send_zy(i):
        wait_bytes(T1.at[pl.ds(0, 2), pl.ds(0, 3)], xs1.at[i])
        for zb in (2 * i, 2 * i + 1):
            if zb:
                remote(T1.at[zb], Xr.at[zb], ssx.at[1], xs2.at[zb], dev(lax.rem(z + ZY[zb][0], 4), yo if ZY[zb][1] else y, xx, c)).start()

    def columns():
        for m in range(2):
            dT[m] = jnp.broadcast_to(dest[m], (128, TOK)).T
            gT[m] = jnp.broadcast_to(gate_ref[m], (128, TOK)).T

        @pl.loop(0, 4)
        def _(r):
            acc[pl.ds(2 * r, 2)] = jnp.zeros((2, 4 * ROWS, D), jnp.float32)

    def mlp(k, j, r):
        rows = Xr[pl.ds(r * 2, 2)].reshape(8 * ROWS, D)
        gate_pre = jnp.dot(rows, W[k, j, 0].reshape(D, fc), preferred_element_type=jnp.float32)
        up_pre = jnp.dot(rows, W[k, j, 1].reshape(D, fc), preferred_element_type=jnp.float32)
        hidden = (jax.nn.silu(gate_pre) * up_pre).astype(jnp.bfloat16)
        return lax.dot_general(hidden, W[k, j, 2].reshape(D, fc), (((1,), (1,)), ((), ())), preferred_element_type=jnp.float32)

    def wait_rows(r):
        for zb in (2 * r, 2 * r + 1):
            if zb:
                wait_bytes(Xr.at[zb], xs2.at[zb])

    def add(r, value):
        acc[pl.ds(2 * r, 2)] += value.reshape(2, 4 * ROWS, D)

    def work(j0, j1, r0, r1):
        nr = r1 - r0

        @pl.loop(0, 2 * (j1 - j0) * nr)
        def _(i):
            r = r0 + lax.rem(i, nr)
            q = lax.div(i, nr)
            add(r, mlp(lax.rem(q, 2), j0 + lax.div(q, 2), r))

    ops.update(P=prep, X=send_x, U=send_zy, Z=columns, R=wait_rows, K=work)
    run(SCHED)
    wait_bytes(S.at[:, pl.ds(0, 3)], ssx.at[0])
    wait_bytes(T1.at[pl.ds(0, 7)], ssx.at[1])

    def back_x(zb):
        if zb:
            wait_bytes(R1.at[zb], rs1.at[zb])
        for dx in (1, 3, 2):
            remote(R1.at[zb, dx], B.at[zb, dx], ssx.at[3], rs2.at[zb], dev(z, y, lax.rem(xx + 4 - dx, 4), c)).start()
        B[zb, 0] = R1[zb, 0]

    def halves(h0, h1, r):
        if h1 > h0:
            @pl.loop(h0, h1)
            def _(h):
                add(r, mlp(lax.bitwise_and(c + h, 1), lax.div(h, 2), r))

    pending = []
    for r in range(4):
        halves(2 * DONE[r], 2 * N_CHUNK - 1, r)
        total = acc[pl.ds(2 * r, 2)].reshape(8 * ROWS, D) + mlp(sib, N_CHUNK - 1, r)
        S[pl.ds(2 * r, 2)] = total.astype(jnp.bfloat16).reshape(2, 4, ROWS, D)
        if r == 0:
            R1[0] = S[0]
        for zb in (2 * r, 2 * r + 1):
            if zb:
                remote(S.at[zb], R1.at[zb], ssx.at[2], rs1.at[zb],
                       dev(lax.rem(z + 4 - ZY[zb][0], 4), yo if ZY[zb][1] else y, xx, c)).start()
        for zb in pending:
            back_x(zb)
        pending = [2 * r, 2 * r + 1]

    def combine(half, first):
        for zb in half:
            wait_bytes(B.at[zb, pl.ds(1, 3)], rs2.at[zb])
        lo = min(half) // 4
        for m in range(2):
            for q in range(2):
                back = B[pl.ds(lo * 4 + q * 2, 2)].reshape(8, ROWS, D).astype(jnp.float32)[:, m * CAP:(m + 1) * CAP].reshape(4, ROWS, D)
                Xr[m * 2 + q] = back.astype(jnp.bfloat16)

        @pl.loop(0, 8)
        def _(n):
            m, i = lax.div(n, 4), lax.rem(n, 4)
            at = pl.ds(pl.multiple_of(i * 256, 256), 256)
            dest_col = dT[m, at]
            pick = jnp.concatenate(
                [(dest_col == (lax.broadcasted_iota(jnp.int32, (256, 128), 1) + 128 * (v + 5 * lo)).astype(jnp.float32)).astype(jnp.bfloat16)
                 for v in range(5)], axis=1)
            back = Xr[pl.ds(m * 2, 2)].reshape(N_EXP * CAP // 2, D)
            mixed = jnp.dot(pick, back, preferred_element_type=jnp.float32)
            if first:
                acc[n, pl.ds(0, 256)] = mixed
            else:
                weight = jnp.concatenate([gT[m, at]] * (D // 128), axis=1)
                y_ref[m, at] = (x_ref[m, at].astype(jnp.float32) + weight * (acc[n, pl.ds(0, 256)] + mixed)).astype(jnp.bfloat16)

    combine((0, 1, 2, 3), True)
    for zb in pending:
        back_x(zb)
    combine((4, 5, 6, 7), False)

    has_local = lax.div(z, 2) == c
    for t, w in enumerate((wg, wu, wd)):
        @pl.when(has_local)
        def _():
            wait_bytes(w.at[pl.ds(0, 3)], ss1.at[t])

        @pl.when(jnp.logical_not(has_local))
        def _():
            wait_bytes(w, ss1.at[t])
    wait_bytes(ST, ss2.at[0])
    wait_bytes(W.at[0, :, :, :, pl.ds(0, 2)], ss2.at[1])
    wait_bytes(W.at[0], ss2.at[2])
    wait_bytes(S.at[pl.ds(0, 7)], ssx.at[2])
    wait_bytes(R1.at[:, pl.ds(0, 3)], ssx.at[3])


def solution(mesh):
    row_spec = P(None, ('rep', 'expert', 'data'), None)
    up_spec = P('expert', 'data', None)
    down_spec = P('expert', None, 'data')
    fc = HALF // N_CHUNK
    bf16 = jnp.bfloat16

    def per_device(x_loc, idx_loc, gate_loc, wg_loc, wu_loc, wd_loc):
        vmem = pl.BlockSpec(memory_space=pltpu.VMEM)
        hbm = pl.BlockSpec(memory_space=pl.ANY)
        dma = pltpu.SemaphoreType.DMA
        return pl.pallas_call(
            moe_kernel,
            out_shape=jax.ShapeDtypeStruct((2, TOK, D), bf16),
            in_specs=[vmem, vmem, vmem, hbm, hbm, hbm],
            out_specs=vmem,
            scratch_shapes=[
                pltpu.VMEM((2, N_CHUNK, 3, 4, 4, SL, fc), bf16),
                pltpu.VMEM((N_CHUNK, 3, 4, SL, fc), bf16),
                pltpu.VMEM((8, 4, ROWS, D), bf16),
                pltpu.VMEM((8, 4, ROWS, D), bf16),
                pltpu.VMEM((8, 4, ROWS, D), bf16),
                pltpu.VMEM((8, 4, ROWS, D), bf16),
                pltpu.VMEM((8, 4 * ROWS, D), jnp.float32),
                pltpu.VMEM((8, 4, ROWS, D), bf16),
                pltpu.VMEM((2, TOK, 128), jnp.float32),
                pltpu.VMEM((2, TOK, 128), jnp.float32),
                dma((2, N_CHUNK)), dma((3, N_CHUNK)), dma((N_CHUNK,)), dma((4,)), dma((8,)), dma((8,)), dma((8,)),
                dma((3,)), dma((3,)), dma((4,)),
            ],
            compiler_params=pltpu.CompilerParams(collective_id=0, has_side_effects=True, vmem_limit_bytes=67043328),
            name='moe',
        )(x_loc, idx_loc.reshape(2, 1, TOK), gate_loc.reshape(2, 1, TOK), wg_loc, wu_loc, wd_loc.transpose(0, 2, 1))

    return jax.shard_map(per_device, mesh=mesh, in_specs=(row_spec, row_spec, row_spec, up_spec, up_spec, down_spec), out_specs=row_spec, check_vma=False)
```

```python
import functools

import jax
import jax.numpy as jnp
from jax import lax
from jax.experimental import pallas as pl
from jax.experimental.pallas import tpu as pltpu
from jax.sharding import PartitionSpec as P

MESH = pl.DeviceIdType.MESH
N_CHUNK = 6
N_EXP = 32
CAP = 40
ROWS = 2 * CAP
D = 768
ZY = ((0, 0), (2, 1), (1, 0), (3, 1), (3, 0), (1, 1), (0, 1), (2, 0))
HEAD = ('W0', 'W1', 'W2', 'W3', 'W4', 'W5')
SCHED = (
    'P0', 'X0', 'P1', 'X1', 'A0', 'P2', 'X2', 'A1', 'P3', 'X3', 'Z', 'C0', 'B0', 'A2', 'C1', 'B1', 'A3', 'U0', 'D0',
    'B2', 'A4', 'U1', 'C2', 'B3', 'A5', 'U2', 'E0', 'D1', 'B4', 'U3', 'C3', 'B5', 'R0', 'K0101', 'E1', 'K1201', 'D2',
    'C4', 'E2', 'K2301', 'D3', 'C5', 'E3', 'K3401', 'D4', 'E4', 'K4501', 'R1', 'K0212', 'D5', 'R2', 'R3', 'E5',
)
DONE = (5, 2, 0, 0)
FF = 3072
HALF = FF // 2
TOK = 1024
SL = 48


def moe_kernel(x_ref, idx_ref, gate_ref, wg, wu, wd, y_ref,
               W, ST, S, T1, Xr, acc, B, dT, gT,
               s1, s2, s3, xs1, xs2, rs, ss1, ss2, ssx):
    fc = HALF // N_CHUNK
    d = lax.axis_index('data')
    g = lax.axis_index('expert')
    z, y = lax.div(d, 4), lax.rem(d, 4)
    xx, c = lax.div(g, 2), lax.rem(g, 2)
    own_p = lax.div(y, 2)
    yo = 3 - y
    yi = y + 1 - 2 * lax.rem(y, 2)
    sib = 1 - c

    def dev(zv, yv, xv, cv):
        return {'data': zv * 4 + yv, 'expert': xv * 2 + cv}

    def remote(src, dst, send, recv, to):
        return pltpu.make_async_remote_copy(src_ref=src, dst_ref=dst, send_sem=send, recv_sem=recv, device_id=to, device_id_type=MESH)

    def wait_bytes(ref, sem):
        pltpu.make_async_copy(ref, ref, sem).wait()

    bsem = pltpu.get_barrier_semaphore()
    n_peer = 4 * len(ZY) - 1
    for zb, (dz, b) in enumerate(ZY):
        for dx in range(4):
            if zb or dx:
                pl.semaphore_signal(bsem, inc=1, device_id=dev(lax.rem(z + dz, 4), yo if b else y, lax.rem(xx + dx, 4), c), device_id_type=MESH)
    for dz in range(4):
        pl.semaphore_signal(bsem, inc=1, device_id=dev(lax.rem(z + dz, 4), y, xx, sib), device_id_type=MESH)
        n_peer += 1
    pl.semaphore_signal(bsem, inc=1, device_id=dev(z, yi, xx, c), device_id_type=MESH)
    n_peer += 1
    pl.semaphore_wait(bsem, n_peer)

    def send_w(j):
        for a in range(2):
            zt = 2 * c + a
            for o in range(2):
                l = 2 * a + (1 - own_p if o else own_p)
                for k in range(2):
                    local = jnp.logical_and(zt == z, c == k)
                    for t, w in enumerate((wg, wu, wd)):
                        src = w.at[l, :, pl.ds(k * HALF + j * fc, fc)]
                        dst = ST.at[j, t, z] if o else W.at[k, j, t, z, y]

                        @pl.when(local)
                        def _():
                            pltpu.make_async_copy(src, dst, s1.at[o, j]).start()

                        @pl.when(jnp.logical_not(local))
                        def _():
                            remote(src, dst, ss1.at[t], s1.at[o, j], dev(zt, y, xx, k)).start()

    def col(j, yv):
        return W.at[c, j, :, :, yv]

    def to_sib(j, yv):
        remote(col(j, yv), col(j, yv), ss2.at[2], s3.at[j], dev(z, y, xx, sib)).start()

    def step_a(j):
        wait_bytes(ST.at[j], s1.at[1, j])
        remote(ST.at[j], col(j, y), ss2.at[0], s2.at[0, j], dev(z, yo, xx, c)).start()
        wait_bytes(col(j, y), s1.at[0, j])
        remote(col(j, y), col(j, y), ss2.at[1], s2.at[1, j], dev(z, yi, xx, c)).start()
        to_sib(j, y)

    def step_b(j):
        wait_bytes(col(j, yo), s2.at[0, j])
        remote(col(j, yo), col(j, yo), ss2.at[1], s2.at[2, j], dev(z, yi, xx, c)).start()
        to_sib(j, yo)

    def step_c(j):
        wait_bytes(col(j, yi), s2.at[1, j])
        to_sib(j, yi)

    def step_d(j):
        wait_bytes(col(j, 3 - yi), s2.at[2, j])
        to_sib(j, 3 - yi)

    def step_e(j):
        wait_bytes(W.at[sib, j], s3.at[j])

    ops = dict(W=send_w, A=step_a, B=step_b, C=step_c, D=step_d, E=step_e)

    def run(plan):
        for word in plan:
            ops[word[0]](*[int(v) for v in word[1:]])

    run(HEAD)

    earlier = (lax.broadcasted_iota(jnp.int32, (TOK, TOK), 0) < lax.broadcasted_iota(jnp.int32, (TOK, TOK), 1)).astype(jnp.bfloat16)
    dest = []
    for m in range(2):
        e = idx_ref[m]
        step_x = lax.bitwise_and(lax.shift_right_logical(e, 3) - xx, 3)
        step_z = lax.bitwise_and(lax.shift_right_logical(e, 1) - z, 3)
        other = lax.bitwise_and(e + own_p, 1)
        ids = step_x
        for zb, (dz, b) in enumerate(ZY):
            ids = ids + jnp.where(step_z * 2 + other == dz * 2 + b, 4 * zb, 0)
        hot = (lax.broadcasted_iota(jnp.int32, (N_EXP, TOK), 0) == ids).astype(jnp.float32)
        before = jnp.dot(hot.astype(jnp.bfloat16), earlier, preferred_element_type=jnp.float32)
        slot = jnp.sum(hot * before, axis=0, keepdims=True)
        kept = slot < CAP
        dest.append(jnp.where(kept, ids.astype(jnp.float32) * CAP + slot, -1.0))
    def prep(i):
        parts = []
        for m in range(2):
            pos = (lax.broadcasted_iota(jnp.int32, (8 * CAP, TOK), 0) + i * (8 * CAP)).astype(jnp.float32)
            pick = (pos == dest[m]).astype(jnp.bfloat16)
            parts.append(jnp.dot(pick, x_ref[m], preferred_element_type=jnp.float32).reshape(8, CAP, D))
        rows = jnp.concatenate(parts, axis=1).astype(jnp.bfloat16).reshape(2, 4, ROWS, D)
        S[pl.ds(2 * i, 2)] = rows
        if i:
            T1[pl.ds(2 * i, 2), 0] = rows[:, 0]
        else:
            Xr[0, 0] = rows[0, 0]
            T1[1, 0] = rows[1, 0]

    def send_x(i):
        for zb in (2 * i, 2 * i + 1):
            for dx in (1, 3, 2):
                land = T1 if zb else Xr
                remote(S.at[zb, dx], land.at[zb, dx], ssx.at[0], xs1.at[i], dev(z, y, lax.rem(xx + dx, 4), c)).start()

    def send_zy(i):
        wait_bytes(T1.at[pl.ds(0, 2), pl.ds(0, 3)], xs1.at[i])
        for zb in (2 * i, 2 * i + 1):
            if zb:
                remote(T1.at[zb], Xr.at[zb], ssx.at[1], xs2.at[zb], dev(lax.rem(z + ZY[zb][0], 4), yo if ZY[zb][1] else y, xx, c)).start()

    def columns():
        for m in range(2):
            dT[m] = jnp.broadcast_to(dest[m], (128, TOK)).T
            gT[m] = jnp.broadcast_to(gate_ref[m], (128, TOK)).T

        @pl.loop(0, 4)
        def _(r):
            acc[pl.ds(2 * r, 2)] = jnp.zeros((2, 4 * ROWS, D), jnp.float32)

    def mlp(k, j, r):
        rows = Xr[pl.ds(r * 2, 2)].reshape(8 * ROWS, D)
        gate_pre = jnp.dot(rows, W[k, j, 0].reshape(D, fc), preferred_element_type=jnp.float32)
        up_pre = jnp.dot(rows, W[k, j, 1].reshape(D, fc), preferred_element_type=jnp.float32)
        hidden = (jax.nn.silu(gate_pre) * up_pre).astype(jnp.bfloat16)
        return lax.dot_general(hidden, W[k, j, 2].reshape(D, fc), (((1,), (1,)), ((), ())), preferred_element_type=jnp.float32)

    def wait_rows(r):
        for zb in (2 * r, 2 * r + 1):
            if zb:
                wait_bytes(Xr.at[zb], xs2.at[zb])

    def add(r, value):
        acc[pl.ds(2 * r, 2)] += value.reshape(2, 4 * ROWS, D)

    def work(j0, j1, r0, r1):
        nr = r1 - r0

        @pl.loop(0, 2 * (j1 - j0) * nr)
        def _(i):
            r = r0 + lax.rem(i, nr)
            q = lax.div(i, nr)
            add(r, mlp(lax.rem(q, 2), j0 + lax.div(q, 2), r))

    ops.update(P=prep, X=send_x, U=send_zy, Z=columns, R=wait_rows, K=work)
    run(SCHED)
    wait_bytes(S.at[:, pl.ds(0, 3)], ssx.at[0])
    wait_bytes(T1.at[pl.ds(0, 7)], ssx.at[1])

    def halves(h0, h1, r):
        if h1 > h0:
            @pl.loop(h0, h1)
            def _(h):
                add(r, mlp(lax.bitwise_and(c + h, 1), lax.div(h, 2), r))

    for r in range(4):
        halves(2 * DONE[r], 2 * N_CHUNK - 1, r)
        total = acc[pl.ds(2 * r, 2)].reshape(8 * ROWS, D) + mlp(sib, N_CHUNK - 1, r)
        S[pl.ds(2 * r, 2)] = total.astype(jnp.bfloat16).reshape(2, 4, ROWS, D)
        for zb in (2 * r, 2 * r + 1):
            z_to, y_to = lax.rem(z + 4 - ZY[zb][0], 4), yo if ZY[zb][1] else y
            for dx in (2, 1, 3, 0):
                if zb or dx:
                    remote(S.at[zb, dx], B.at[zb, dx], ssx.at[2 if zb else 3], rs.at[zb], dev(z_to, y_to, lax.rem(xx + 4 - dx, 4), c)).start()
                else:
                    B[0, 0] = S[0, 0]

    def combine(half, first):
        for zb in half:
            wait_bytes(B.at[zb] if zb else B.at[0, pl.ds(1, 3)], rs.at[zb])
        lo = min(half) // 4
        for m in range(2):
            for q in range(2):
                back = B[pl.ds(lo * 4 + q * 2, 2)].reshape(8, ROWS, D).astype(jnp.float32)[:, m * CAP:(m + 1) * CAP].reshape(4, ROWS, D)
                Xr[m * 2 + q] = back.astype(jnp.bfloat16)

        @pl.loop(0, 8)
        def _(n):
            m, i = lax.div(n, 4), lax.rem(n, 4)
            at = pl.ds(pl.multiple_of(i * 256, 256), 256)
            dest_col = dT[m, at]
            pick = jnp.concatenate(
                [(dest_col == (lax.broadcasted_iota(jnp.int32, (256, 128), 1) + 128 * (v + 5 * lo)).astype(jnp.float32)).astype(jnp.bfloat16)
                 for v in range(5)], axis=1)
            back = Xr[pl.ds(m * 2, 2)].reshape(N_EXP * CAP // 2, D)
            mixed = jnp.dot(pick, back, preferred_element_type=jnp.float32)
            if first:
                acc[n, pl.ds(0, 256)] = mixed
            else:
                weight = jnp.concatenate([gT[m, at]] * (D // 128), axis=1)
                y_ref[m, at] = (x_ref[m, at].astype(jnp.float32) + weight * (acc[n, pl.ds(0, 256)] + mixed)).astype(jnp.bfloat16)

    combine((0, 1, 2, 3), True)
    combine((4, 5, 6, 7), False)

    has_local = lax.div(z, 2) == c
    for t, w in enumerate((wg, wu, wd)):
        @pl.when(has_local)
        def _():
            wait_bytes(w.at[pl.ds(0, 3)], ss1.at[t])

        @pl.when(jnp.logical_not(has_local))
        def _():
            wait_bytes(w, ss1.at[t])
    wait_bytes(ST, ss2.at[0])
    wait_bytes(W.at[0, :, :, :, pl.ds(0, 2)], ss2.at[1])
    wait_bytes(W.at[0], ss2.at[2])
    wait_bytes(S.at[pl.ds(1, 7)], ssx.at[2])
    wait_bytes(S.at[0, pl.ds(1, 3)], ssx.at[3])


def solution(mesh):
    row_spec = P(None, ('rep', 'expert', 'data'), None)
    up_spec = P('expert', 'data', None)
    down_spec = P('expert', None, 'data')
    fc = HALF // N_CHUNK
    bf16 = jnp.bfloat16

    def per_device(x_loc, idx_loc, gate_loc, wg_loc, wu_loc, wd_loc):
        vmem = pl.BlockSpec(memory_space=pltpu.VMEM)
        hbm = pl.BlockSpec(memory_space=pl.ANY)
        dma = pltpu.SemaphoreType.DMA
        return pl.pallas_call(
            moe_kernel,
            out_shape=jax.ShapeDtypeStruct((2, TOK, D), bf16),
            in_specs=[vmem, vmem, vmem, hbm, hbm, hbm],
            out_specs=vmem,
            scratch_shapes=[
                pltpu.VMEM((2, N_CHUNK, 3, 4, 4, SL, fc), bf16),
                pltpu.VMEM((N_CHUNK, 3, 4, SL, fc), bf16),
                pltpu.VMEM((8, 4, ROWS, D), bf16),
                pltpu.VMEM((8, 4, ROWS, D), bf16),
                pltpu.VMEM((8, 4, ROWS, D), bf16),
                pltpu.VMEM((8, 4 * ROWS, D), jnp.float32),
                pltpu.VMEM((8, 4, ROWS, D), bf16),
                pltpu.VMEM((2, TOK, 128), jnp.float32),
                pltpu.VMEM((2, TOK, 128), jnp.float32),
                dma((2, N_CHUNK)), dma((3, N_CHUNK)), dma((N_CHUNK,)), dma((4,)), dma((8,)), dma((8,)),
                dma((3,)), dma((3,)), dma((4,)),
            ],
            compiler_params=pltpu.CompilerParams(collective_id=0, has_side_effects=True, vmem_limit_bytes=67043328),
            name='moe',
        )(x_loc, idx_loc.reshape(2, 1, TOK), gate_loc.reshape(2, 1, TOK), wg_loc, wu_loc, wd_loc.transpose(0, 2, 1))

    return jax.shard_map(per_device, mesh=mesh, in_specs=(row_spec, row_spec, row_spec, up_spec, up_spec, down_spec), out_specs=row_spec, check_vma=False)
```

```python
import functools

import jax
import jax.numpy as jnp
from jax import lax
from jax.experimental import pallas as pl
from jax.experimental.pallas import tpu as pltpu
from jax.sharding import PartitionSpec as P

MESH = pl.DeviceIdType.MESH
N_CHUNK = 6
N_EXP = 32
CAP = 40
ROWS = 2 * CAP
D = 768
ZY = ((0, 0), (2, 1), (1, 0), (3, 1), (3, 0), (1, 1), (0, 1), (2, 0))
HEAD = ('W0', 'W1', 'W2', 'W3', 'W4', 'W5')
SCHED = (
    'P0', 'X0', 'P1', 'X1', 'A0', 'P2', 'X2', 'A1', 'P3', 'X3', 'Z', 'C0', 'B0', 'A2', 'C1', 'B1', 'A3', 'D0', 'B2',
    'U0', 'A4', 'C2', 'B3', 'U1', 'A5', 'E0', 'D1', 'B4', 'U2', 'C3', 'B5', 'U3', 'R0', 'K0101', 'E1', 'K1201', 'D2',
    'C4', 'E2', 'K2301', 'D3', 'C5', 'E3', 'K3401', 'D4', 'E4', 'K4501', 'R1', 'K0212', 'D5', 'R2', 'R3', 'E5',
)
DONE = (5, 2, 0, 0)
FF = 3072
HALF = FF // 2
TOK = 1024
SL = 48


def moe_kernel(x_ref, idx_ref, gate_ref, wg, wu, wd, y_ref,
               W, ST, S, T1, Xr, acc, B, dT, gT,
               s1, s2, s3, xs1, xs2, rs, ss1, ss2, ssx):
    fc = HALF // N_CHUNK
    d = lax.axis_index('data')
    g = lax.axis_index('expert')
    z, y = lax.div(d, 4), lax.rem(d, 4)
    xx, c = lax.div(g, 2), lax.rem(g, 2)
    own_p = lax.div(y, 2)
    yo = 3 - y
    yi = y + 1 - 2 * lax.rem(y, 2)
    sib = 1 - c

    def dev(zv, yv, xv, cv):
        return {'data': zv * 4 + yv, 'expert': xv * 2 + cv}

    def remote(src, dst, send, recv, to):
        return pltpu.make_async_remote_copy(src_ref=src, dst_ref=dst, send_sem=send, recv_sem=recv, device_id=to, device_id_type=MESH)

    def wait_bytes(ref, sem):
        pltpu.make_async_copy(ref, ref, sem).wait()

    bsem = pltpu.get_barrier_semaphore()
    n_peer = 4 * len(ZY) - 1
    for zb, (dz, b) in enumerate(ZY):
        for dx in range(4):
            if zb or dx:
                pl.semaphore_signal(bsem, inc=1, device_id=dev(lax.rem(z + dz, 4), yo if b else y, lax.rem(xx + dx, 4), c), device_id_type=MESH)
    for dz in range(4):
        pl.semaphore_signal(bsem, inc=1, device_id=dev(lax.rem(z + dz, 4), y, xx, sib), device_id_type=MESH)
        n_peer += 1
    pl.semaphore_signal(bsem, inc=1, device_id=dev(z, yi, xx, c), device_id_type=MESH)
    n_peer += 1
    pl.semaphore_wait(bsem, n_peer)

    def send_w(j):
        for a in range(2):
            zt = 2 * c + a
            for o in range(2):
                l = 2 * a + (1 - own_p if o else own_p)
                for k in range(2):
                    local = jnp.logical_and(zt == z, c == k)
                    for t, w in enumerate((wg, wu, wd)):
                        src = w.at[l, :, pl.ds(k * HALF + j * fc, fc)]
                        dst = ST.at[j, t, z] if o else W.at[k, j, t, z, y]

                        @pl.when(local)
                        def _():
                            pltpu.make_async_copy(src, dst, s1.at[o, j]).start()

                        @pl.when(jnp.logical_not(local))
                        def _():
                            remote(src, dst, ss1.at[t], s1.at[o, j], dev(zt, y, xx, k)).start()

    def col(j, yv):
        return W.at[c, j, :, :, yv]

    def to_sib(j, yv):
        remote(col(j, yv), col(j, yv), ss2.at[2], s3.at[j], dev(z, y, xx, sib)).start()

    def step_a(j):
        wait_bytes(ST.at[j], s1.at[1, j])
        remote(ST.at[j], col(j, y), ss2.at[0], s2.at[0, j], dev(z, yo, xx, c)).start()
        wait_bytes(col(j, y), s1.at[0, j])
        remote(col(j, y), col(j, y), ss2.at[1], s2.at[1, j], dev(z, yi, xx, c)).start()
        to_sib(j, y)

    def step_b(j):
        wait_bytes(col(j, yo), s2.at[0, j])
        remote(col(j, yo), col(j, yo), ss2.at[1], s2.at[2, j], dev(z, yi, xx, c)).start()
        to_sib(j, yo)

    def step_c(j):
        wait_bytes(col(j, yi), s2.at[1, j])
        to_sib(j, yi)

    def step_d(j):
        wait_bytes(col(j, 3 - yi), s2.at[2, j])
        to_sib(j, 3 - yi)

    def step_e(j):
        wait_bytes(W.at[sib, j], s3.at[j])

    ops = dict(W=send_w, A=step_a, B=step_b, C=step_c, D=step_d, E=step_e)

    def run(plan):
        for word in plan:
            ops[word[0]](*[int(v) for v in word[1:]])

    run(HEAD)

    earlier = (lax.broadcasted_iota(jnp.int32, (TOK, TOK), 0) < lax.broadcasted_iota(jnp.int32, (TOK, TOK), 1)).astype(jnp.bfloat16)
    dest = []
    for m in range(2):
        e = idx_ref[m]
        step_x = lax.bitwise_and(lax.shift_right_logical(e, 3) - xx, 3)
        step_z = lax.bitwise_and(lax.shift_right_logical(e, 1) - z, 3)
        other = lax.bitwise_and(e + own_p, 1)
        ids = step_x
        for zb, (dz, b) in enumerate(ZY):
            ids = ids + jnp.where(step_z * 2 + other == dz * 2 + b, 4 * zb, 0)
        hot = (lax.broadcasted_iota(jnp.int32, (N_EXP, TOK), 0) == ids).astype(jnp.float32)
        before = jnp.dot(hot.astype(jnp.bfloat16), earlier, preferred_element_type=jnp.float32)
        slot = jnp.sum(hot * before, axis=0, keepdims=True)
        kept = slot < CAP
        dest.append(jnp.where(kept, ids.astype(jnp.float32) * CAP + slot, -1.0))
    def prep(i):
        parts = []
        for m in range(2):
            pos = (lax.broadcasted_iota(jnp.int32, (8 * CAP, TOK), 0) + i * (8 * CAP)).astype(jnp.float32)
            pick = (pos == dest[m]).astype(jnp.bfloat16)
            parts.append(jnp.dot(pick, x_ref[m], preferred_element_type=jnp.float32).reshape(8, CAP, D))
        rows = jnp.concatenate(parts, axis=1).astype(jnp.bfloat16).reshape(2, 4, ROWS, D)
        S[pl.ds(2 * i, 2)] = rows
        if i:
            T1[pl.ds(2 * i, 2), 0] = rows[:, 0]
        else:
            Xr[0, 0] = rows[0, 0]
            T1[1, 0] = rows[1, 0]

    def send_x(i):
        for zb in (2 * i, 2 * i + 1):
            for dx in (1, 3, 2):
                land = T1 if zb else Xr
                remote(S.at[zb, dx], land.at[zb, dx], ssx.at[0], xs1.at[i], dev(z, y, lax.rem(xx + dx, 4), c)).start()

    def send_zy(i):
        wait_bytes(T1.at[pl.ds(0, 2), pl.ds(0, 3)], xs1.at[i])
        for zb in (2 * i, 2 * i + 1):
            if zb:
                remote(T1.at[zb], Xr.at[zb], ssx.at[1], xs2.at[zb], dev(lax.rem(z + ZY[zb][0], 4), yo if ZY[zb][1] else y, xx, c)).start()

    def columns():
        for m in range(2):
            dT[m] = jnp.broadcast_to(dest[m], (128, TOK)).T
            gT[m] = jnp.broadcast_to(gate_ref[m], (128, TOK)).T

        @pl.loop(0, 4)
        def _(r):
            acc[pl.ds(2 * r, 2)] = jnp.zeros((2, 4 * ROWS, D), jnp.float32)

    def mlp(k, j, r):
        rows = Xr[pl.ds(r * 2, 2)].reshape(8 * ROWS, D)
        gate_pre = jnp.dot(rows, W[k, j, 0].reshape(D, fc), preferred_element_type=jnp.float32)
        up_pre = jnp.dot(rows, W[k, j, 1].reshape(D, fc), preferred_element_type=jnp.float32)
        hidden = (jax.nn.silu(gate_pre) * up_pre).astype(jnp.bfloat16)
        return lax.dot_general(hidden, W[k, j, 2].reshape(D, fc), (((1,), (1,)), ((), ())), preferred_element_type=jnp.float32)

    def wait_rows(r):
        for zb in (2 * r, 2 * r + 1):
            if zb:
                wait_bytes(Xr.at[zb], xs2.at[zb])

    def add(r, value):
        acc[pl.ds(2 * r, 2)] += value.reshape(2, 4 * ROWS, D)

    def work(j0, j1, r0, r1):
        nr = r1 - r0

        @pl.loop(0, 2 * (j1 - j0) * nr)
        def _(i):
            r = r0 + lax.rem(i, nr)
            q = lax.div(i, nr)
            add(r, mlp(lax.rem(q, 2), j0 + lax.div(q, 2), r))

    ops.update(P=prep, X=send_x, U=send_zy, Z=columns, R=wait_rows, K=work)
    run(SCHED)
    wait_bytes(S.at[:, pl.ds(0, 3)], ssx.at[0])
    wait_bytes(T1.at[pl.ds(0, 7)], ssx.at[1])

    def halves(h0, h1, r):
        if h1 > h0:
            @pl.loop(h0, h1)
            def _(h):
                add(r, mlp(lax.bitwise_and(c + h, 1), lax.div(h, 2), r))

    for r in range(4):
        halves(2 * DONE[r], 2 * N_CHUNK - 1, r)
        total = acc[pl.ds(2 * r, 2)].reshape(8 * ROWS, D) + mlp(sib, N_CHUNK - 1, r)
        S[pl.ds(2 * r, 2)] = total.astype(jnp.bfloat16).reshape(2, 4, ROWS, D)
        for zb in (2 * r, 2 * r + 1):
            z_to, y_to = lax.rem(z + 4 - ZY[zb][0], 4), yo if ZY[zb][1] else y
            for dx in (2, 1, 3, 0):
                if zb or dx:
                    remote(S.at[zb, dx], B.at[zb, dx], ssx.at[2 if zb else 3], rs.at[zb], dev(z_to, y_to, lax.rem(xx + 4 - dx, 4), c)).start()
                else:
                    B[0, 0] = S[0, 0]

    def combine(half, first):
        for zb in half:
            wait_bytes(B.at[zb] if zb else B.at[0, pl.ds(1, 3)], rs.at[zb])
        lo = min(half) // 4
        for m in range(2):
            for q in range(2):
                back = B[pl.ds(lo * 4 + q * 2, 2)].reshape(8, ROWS, D).astype(jnp.float32)[:, m * CAP:(m + 1) * CAP].reshape(4, ROWS, D)
                Xr[m * 2 + q] = back.astype(jnp.bfloat16)

        @pl.loop(0, 8)
        def _(n):
            m, i = lax.div(n, 4), lax.rem(n, 4)
            at = pl.ds(pl.multiple_of(i * 256, 256), 256)
            dest_col = dT[m, at]
            pick = jnp.concatenate(
                [(dest_col == (lax.broadcasted_iota(jnp.int32, (256, 128), 1) + 128 * (v + 5 * lo)).astype(jnp.float32)).astype(jnp.bfloat16)
                 for v in range(5)], axis=1)
            back = Xr[pl.ds(m * 2, 2)].reshape(N_EXP * CAP // 2, D)
            mixed = jnp.dot(pick, back, preferred_element_type=jnp.float32)
            if first:
                acc[n, pl.ds(0, 256)] = mixed
            else:
                weight = jnp.concatenate([gT[m, at]] * (D // 128), axis=1)
                y_ref[m, at] = (x_ref[m, at].astype(jnp.float32) + weight * (acc[n, pl.ds(0, 256)] + mixed)).astype(jnp.bfloat16)

    combine((0, 1, 2, 3), True)
    combine((4, 5, 6, 7), False)

    has_local = lax.div(z, 2) == c
    for t, w in enumerate((wg, wu, wd)):
        @pl.when(has_local)
        def _():
            wait_bytes(w.at[pl.ds(0, 3)], ss1.at[t])

        @pl.when(jnp.logical_not(has_local))
        def _():
            wait_bytes(w, ss1.at[t])
    wait_bytes(ST, ss2.at[0])
    wait_bytes(W.at[0, :, :, :, pl.ds(0, 2)], ss2.at[1])
    wait_bytes(W.at[0], ss2.at[2])
    wait_bytes(S.at[pl.ds(1, 7)], ssx.at[2])
    wait_bytes(S.at[0, pl.ds(1, 3)], ssx.at[3])


def solution(mesh):
    row_spec = P(None, ('rep', 'expert', 'data'), None)
    up_spec = P('expert', 'data', None)
    down_spec = P('expert', None, 'data')
    fc = HALF // N_CHUNK
    bf16 = jnp.bfloat16

    def per_device(x_loc, idx_loc, gate_loc, wg_loc, wu_loc, wd_loc):
        vmem = pl.BlockSpec(memory_space=pltpu.VMEM)
        hbm = pl.BlockSpec(memory_space=pl.ANY)
        dma = pltpu.SemaphoreType.DMA
        return pl.pallas_call(
            moe_kernel,
            out_shape=jax.ShapeDtypeStruct((2, TOK, D), bf16),
            in_specs=[vmem, vmem, vmem, hbm, hbm, hbm],
            out_specs=vmem,
            scratch_shapes=[
                pltpu.VMEM((2, N_CHUNK, 3, 4, 4, SL, fc), bf16),
                pltpu.VMEM((N_CHUNK, 3, 4, SL, fc), bf16),
                pltpu.VMEM((8, 4, ROWS, D), bf16),
                pltpu.VMEM((8, 4, ROWS, D), bf16),
                pltpu.VMEM((8, 4, ROWS, D), bf16),
                pltpu.VMEM((8, 4 * ROWS, D), jnp.float32),
                pltpu.VMEM((8, 4, ROWS, D), bf16),
                pltpu.VMEM((2, TOK, 128), jnp.float32),
                pltpu.VMEM((2, TOK, 128), jnp.float32),
                dma((2, N_CHUNK)), dma((3, N_CHUNK)), dma((N_CHUNK,)), dma((4,)), dma((8,)), dma((8,)),
                dma((3,)), dma((3,)), dma((4,)),
            ],
            compiler_params=pltpu.CompilerParams(collective_id=0, has_side_effects=True, vmem_limit_bytes=67043328),
            name='moe',
        )(x_loc, idx_loc.reshape(2, 1, TOK), gate_loc.reshape(2, 1, TOK), wg_loc, wu_loc, wd_loc.transpose(0, 2, 1))

    return jax.shard_map(per_device, mesh=mesh, in_specs=(row_spec, row_spec, row_spec, up_spec, up_spec, down_spec), out_specs=row_spec, check_vma=False)
```
